32 devices in a mesh: dp: 1 (over z), cx: 4 (over y), cy: 8 (over x, core).
Axes of the slice: x: 4, y: 4, z: 1, core: 2. Of those that a mesh axis runs over, the one named last changes fastest.
The devices are a block of a 4x4x8 slice.
Arguments:
- x: bfloat16 [1, 2048, 3072], P('dp', ('cx', 'cy'))
- w_qkv: bfloat16 [3072, 9216], replicated
- w_o: bfloat16 [48, 64, 3072], replicated
Outputs:
- output: bfloat16 [1, 2048, 3072], P('dp', ('cx', 'cy'))
All inputs are finite; a program needn't handle non-finite values.
Results may differ from the reference program's by a relative error of at most 0.0080538.
Values are sent between devices in bfloat16 or wider.
A program may use at most 768 MiB of HBM per device.

```python
import math
import jax
import jax.numpy as jnp
from jax import lax

SEQ_LEN = 2048
NUM_HEADS = 48
HEAD_DIM = 64


def setup_inputs(seed: int = 0, part: int = 0) -> dict:
    model_width = NUM_HEADS * HEAD_DIM
    base_key = jax.random.key(seed)
    token_key = jax.random.fold_in(jax.random.fold_in(base_key, part), 1)
    qkv_key = jax.random.fold_in(base_key, 2)
    out_key = jax.random.fold_in(base_key, 3)
    logit_std = math.sqrt(max(math.log(SEQ_LEN / 20.0), 2.0))
    qk_gain = math.sqrt(logit_std)
    col_gain = jnp.concatenate([jnp.full((2 * model_width,), qk_gain, jnp.float32), jnp.ones((model_width,), jnp.float32)])
    tokens = jax.random.normal(token_key, (1, SEQ_LEN, model_width), jnp.float32)
    w_qkv = jax.random.normal(qkv_key, (model_width, 3 * model_width), jnp.float32) * (model_width ** -0.5) * col_gain
    w_out = jax.random.normal(out_key, (NUM_HEADS, HEAD_DIM, model_width), jnp.float32) * (2.5 * model_width ** -0.5)
    return {"x": tokens.astype(jnp.bfloat16), "w_qkv": w_qkv.astype(jnp.bfloat16), "w_o": w_out.astype(jnp.bfloat16)}


def reference(x, w_qkv, w_o):
    model_width = NUM_HEADS * HEAD_DIM
    q_block = math.gcd(SEQ_LEN, 256)
    n_blocks = SEQ_LEN // q_block
    inv_sqrt = 1.0 / math.sqrt(HEAD_DIM)
    qkv_rows = jnp.dot(x[0], w_qkv, preferred_element_type=jnp.float32).astype(jnp.bfloat16)
    qkv_rows = jnp.transpose(qkv_rows.reshape(SEQ_LEN, 3, NUM_HEADS, HEAD_DIM), (1, 2, 0, 3))

    def head_attend(head_args):
        q_head, k_head, v_head = head_args
        k_full = k_head.astype(jnp.float32)
        v_full = v_head.astype(jnp.float32)
        q_blocks = q_head.astype(jnp.float32).reshape(n_blocks, q_block, HEAD_DIM)

        def block_attend(q_rows):
            logits = jnp.dot(q_rows, k_full.T, preferred_element_type=jnp.float32) * inv_sqrt
            row_max = jnp.max(logits, axis=-1, keepdims=True)
            weights = jnp.exp(logits - row_max)
            row_sum = jnp.sum(weights, axis=-1, keepdims=True)
            return jnp.dot(weights, v_full, preferred_element_type=jnp.float32) / row_sum

        return lax.map(block_attend, q_blocks).reshape(SEQ_LEN, HEAD_DIM)

    attn_rows = lax.map(head_attend, (qkv_rows[0], qkv_rows[1], qkv_rows[2]))
    attn_rows = jnp.transpose(attn_rows, (1, 0, 2)).reshape(SEQ_LEN, model_width).astype(jnp.bfloat16)
    result = jnp.dot(attn_rows, w_o.reshape(model_width, model_width), preferred_element_type=jnp.float32)
    return result.astype(jnp.bfloat16)[None]
```

```python
import functools

import jax
import jax.numpy as jnp
from jax import lax
from jax.experimental import pallas as pl
from jax.experimental.pallas import tpu as pltpu
from jax.sharding import PartitionSpec as P

MESH = pl.DeviceIdType.MESH
BF16, F32 = jnp.bfloat16, jnp.float32
LOG2E = 1.4426950408889634


def kernel(cfg, x_ref, w_ref, wo_ref, y_ref, xv, wv, wov, stage, buf, ostage, obuf, acc,
           x_sem, w_sem, wo_sem, xs_sem, xr_sem, qs_sem, qr_sem, fs_sem, fr_sem, os_sem, or_sem):
    n_cx, n_cy, chips, chunks, heads, hd = cfg
    row_chips = n_cy // 2
    half = chips // 2
    rows = x_ref.shape[0]
    width = x_ref.shape[1]
    kv_rows = 2 * rows
    span = half * hd
    scale = hd ** -0.5 * LOG2E

    i = lax.axis_index("cx")
    j = lax.axis_index("cy")
    xx = j // 2
    c = lax.rem(j, 2)
    e = i * row_chips + xx
    par = lax.rem(e, 2)

    def dev(chip, core):
        return {"cx": chip // row_chips, "cy": lax.rem(chip, row_chips) * 2 + core}

    my_rows = pl.ds(pl.multiple_of(c * rows, rows), rows)
    x_in = pltpu.make_async_copy(x_ref, xv.at[my_rows], x_sem)
    x_in.start()

    def w_copy(s, t):
        col = pl.multiple_of((t * heads + s * chips) * hd + c * span, 128)
        return pltpu.make_async_copy(w_ref.at[:, pl.ds(col, span)], wv.at[3 * s + t], w_sem.at[3 * s + t])

    def wo_copy(s):
        part = pl.ds(s * chips * hd, chips * hd)
        return pltpu.make_async_copy(wo_ref.at[part], wov.at[part], wo_sem.at[s])

    for s in range(chunks):
        for t in range(3):
            w_copy(s, t).start()
    for s in range(chunks):
        wo_copy(s).start()

    n_dev = n_cx * n_cy
    barrier = pltpu.get_barrier_semaphore()

    def greet(k, _):
        other = lax.rem(i * n_cy + j + k, n_dev)
        pl.semaphore_signal(barrier, inc=1, device_id={"cx": other // n_cy, "cy": lax.rem(other, n_cy)},
                            device_id_type=MESH)
        return 0

    lax.fori_loop(1, n_dev, greet, 0)
    pl.semaphore_wait(barrier, n_dev - 1)

    x_in.wait()
    x_swap = pltpu.make_async_remote_copy(xv.at[my_rows], xv.at[my_rows], xs_sem, xr_sem,
                                          device_id=dev(e, 1 - c), device_id_type=MESH)
    x_swap.start()
    x_swap.wait()

    lane = lax.broadcasted_iota(jnp.int32, (kv_rows, 128), 1)
    low = lane < hd
    low_q = low[:rows]
    low_o = low[:rows // 2]

    def qkv_send(s, k):
        d = c * half + k
        return pltpu.make_async_remote_copy(stage.at[s, k], buf.at[s, e], qs_sem.at[s, k], qr_sem.at[s, e // 2],
                                            device_id=dev(d, par), device_id_type=MESH)

    def project(s):
        parts = []
        for t in range(3):
            w_copy(s, t).wait()
            parts.append(jnp.dot(xv[...], wv[3 * s + t], preferred_element_type=F32))
        for p in range(half // 2):
            sl = slice(128 * p, 128 * p + 128)
            q, k, v = (a[:, sl] for a in parts)
            q_lo, q_hi = q[:rows], q[rows:]
            stage[s, 2 * p, 0:rows] = jnp.where(low_q, q_lo, pltpu.roll(q_hi, hd, 1)).astype(BF16)
            stage[s, 2 * p + 1, 0:rows] = jnp.where(low_q, pltpu.roll(q_lo, hd, 1), q_hi).astype(BF16)
            stage[s, 2 * p, rows:] = jnp.where(low, k, pltpu.roll(v, hd, 1)).astype(BF16)
            stage[s, 2 * p + 1, rows:] = jnp.where(low, pltpu.roll(k, hd, 1), v).astype(BF16)

        def send(n, _):
            dx = lax.rem(n // 2 + 1 + xx, row_chips)
            k = lax.rem(n, 2) * row_chips + dx
            mine = jnp.logical_and(c * half + k == e, par == c)

            @pl.when(mine)
            def _():
                buf[s, e] = stage[s, k]

            @pl.when(jnp.logical_not(mine))
            def _():
                qkv_send(s, k).start()
            return 0

        lax.fori_loop(0, half, send, 0)

    def sent(s):
        def one(k, _):
            @pl.when(jnp.logical_not(jnp.logical_and(c * half + k == e, par == c)))
            def _():
                qkv_send(s, k).wait_send()
            return 0

        lax.fori_loop(0, half, one, 0)

    def fwd(s, n, core):
        part = buf.at[s, 2 * n + core, pl.ds(rows, kv_rows)]
        return pltpu.make_async_remote_copy(part, part, fs_sem.at[s, n], fr_sem.at[s, n],
                                            device_id=dev(e, 1 - c), device_id_type=MESH)

    def forward(s):
        def one(n, _):
            src = 2 * n + c
            local = jnp.logical_and(src == e, e // half == c)

            @pl.when(jnp.logical_not(local))
            def _():
                pltpu.make_async_remote_copy(buf.at[s, src], buf.at[s, src], qs_sem.at[s, 0], qr_sem.at[s, n],
                                             device_id=dev(e, 1 - c), device_id_type=MESH).wait_recv()
            fwd(s, n, c).start()
            return 0

        lax.fori_loop(0, half, one, 0)

    def o_send(s, n, core):
        q_chip = 2 * n + c
        return pltpu.make_async_remote_copy(ostage.at[s, 2 * n + core], obuf.at[s, e], os_sem.at[s, 2 * n + core],
                                            or_sem.at[s, e], device_id=dev(q_chip, core), device_id_type=MESH)

    def attend(s):
        def got(n, _):
            fwd(s, n, 1 - c).wait_recv()
            return 0

        lax.fori_loop(0, half, got, 0)

        def block(b, _):
            qs = []
            for u in range(2):
                qq = buf[s, 2 * (2 * b + u) + c, 0:rows].astype(F32)
                qs.append(jnp.where(low_q, qq, 0.0).astype(BF16))
                qs.append(jnp.where(low_q, pltpu.roll(qq, hd, 1), 0.0).astype(BF16))
            q = jnp.concatenate(qs, axis=0)
            kv = jnp.concatenate([buf[s, n, rows:] for n in range(chips)], axis=0)
            logits = lax.dot_general(q, kv, (((1,), (1,)), ((), ())), preferred_element_type=F32)
            m = jnp.max(logits, axis=1, keepdims=True)
            w = jnp.exp2((logits - m) * scale)
            den = jnp.sum(w, axis=1, keepdims=True)
            o = jnp.dot(w.astype(BF16), kv, preferred_element_type=F32) / den
            hr = rows // 2
            for u in range(4):
                top, bot = o[u * rows:u * rows + hr], o[u * rows + hr:(u + 1) * rows]
                ostage[s, 4 * b + u] = jnp.where(low_o, pltpu.roll(top, hd, 1), bot).astype(BF16)
            for u in range(4):
                n, core = 2 * b + u // 2, u % 2
                mine = jnp.logical_and(2 * n + c == e, c == core)

                @pl.when(mine)
                def _():
                    obuf[s, e] = ostage[s, 4 * b + u]

                @pl.when(jnp.logical_not(mine))
                def _():
                    o_send(s, n, core).start()
            return 0

        lax.fori_loop(0, half // 2, block, 0)

    def o_sent(s):
        def one(n, _):
            for core in range(2):
                @pl.when(jnp.logical_not(jnp.logical_and(2 * n + c == e, c == core)))
                def _():
                    o_send(s, n, core).wait_send()
            return 0

        lax.fori_loop(0, half, one, 0)

    def output(s):
        def got(d, _):
            @pl.when(jnp.logical_not(jnp.logical_and(d == e, par == c)))
            def _():
                pltpu.make_async_remote_copy(obuf.at[s, d], obuf.at[s, d], os_sem.at[s, 0], or_sem.at[s, d],
                                             device_id=dev(e, 1 - c), device_id_type=MESH).wait_recv()
            return 0

        lax.fori_loop(0, chips, got, 0)
        wo_copy(s).wait()
        tiles = []
        for p in range(half):
            a, b = obuf[s, 2 * p].astype(F32), obuf[s, 2 * p + 1].astype(F32)
            top = jnp.where(low_o, a, pltpu.roll(b, hd, 1))
            bot = jnp.where(low_o, pltpu.roll(a, hd, 1), b)
            tiles.append(jnp.concatenate([top, bot], axis=0).astype(BF16))
        o = jnp.concatenate(tiles, axis=1)
        part = jnp.dot(o, wov[s * chips * hd:(s + 1) * chips * hd], preferred_element_type=F32)
        if s == 0:
            acc[...] = part
        elif s < chunks - 1:
            acc[...] += part
        else:
            y_ref[...] = (acc[...] + part).astype(BF16)

    for s in range(chunks):
        project(s)
    forward(0)
    attend(0)
    forward(1)
    attend(1)
    forward(2)
    output(0)
    attend(2)
    output(1)
    output(2)
    for s in range(chunks):
        sent(s)
        o_sent(s)

        def one(n, _):
            fwd(s, n, c).wait_send()
            return 0

        lax.fori_loop(0, half, one, 0)


def solution(mesh):
    n_cx, n_cy = mesh.shape["cx"], mesh.shape["cy"]
    chips = n_cx * n_cy // 2

    def attend_local(x_blk, w_qkv, w_o):
        heads, hd, width = w_o.shape
        rows = x_blk.shape[1]
        chunks = heads // chips
        half = chips // 2
        dma, vm = pltpu.SemaphoreType.DMA, pltpu.VMEM
        any_ = pl.BlockSpec(memory_space=pl.ANY)
        y = pl.pallas_call(
            functools.partial(kernel, (n_cx, n_cy, chips, chunks, heads, hd)),
            out_shape=jax.ShapeDtypeStruct((rows, width), BF16),
            in_specs=[any_, any_, any_],
            out_specs=pl.BlockSpec(memory_space=pltpu.VMEM),
            scratch_shapes=[
                vm((2 * rows, width), BF16),
                vm((3 * chunks, width, half * hd), BF16),
                vm((heads * hd, width), BF16),
                vm((chunks, half, 3 * rows, 128), BF16),
                vm((chunks, chips, 3 * rows, 128), BF16),
                vm((chunks, chips, rows // 2, 128), BF16),
                vm((chunks, chips, rows // 2, 128), BF16),
                vm((rows, width), F32),
                dma, dma((3 * chunks,)), dma((chunks,)), dma, dma,
                dma((chunks, half)), dma((chunks, half)),
                dma((chunks, half)), dma((chunks, half)),
                dma((chunks, chips)), dma((chunks, chips)),
            ],
            compiler_params=pltpu.CompilerParams(
                collective_id=0, has_side_effects=True, vmem_limit_bytes=63 * 2 ** 20),
        )(x_blk[0], w_qkv, w_o.reshape(heads * hd, width))
        return y[None]

    return jax.shard_map(
        attend_local, mesh=mesh,
        in_specs=(P("dp", ("cx", "cy"), None), P(None, None), P(None, None, None)),
        out_specs=P("dp", ("cx", "cy"), None), check_vma=False)
```

```python
import functools

import jax
import jax.numpy as jnp
from jax import lax
from jax.experimental import pallas as pl
from jax.experimental.pallas import tpu as pltpu
from jax.sharding import PartitionSpec as P

MESH = pl.DeviceIdType.MESH
BF16, F32 = jnp.bfloat16, jnp.float32
LOG2E = 1.4426950408889634


def kernel(cfg, x_ref, w_ref, wo_ref, y_ref, xv, wv, wov, stage, buf, ostage, obuf, acc,
           x_sem, w_sem, wo_sem, xs_sem, xr_sem, qs_sem, qr_sem, fs_sem, fr_sem, os_sem, or_sem):
    n_cx, n_cy, chips, chunks, heads, hd = cfg
    row_chips = n_cy // 2
    half = chips // 2
    rows = x_ref.shape[0]
    width = x_ref.shape[1]
    kv_rows = 2 * rows
    span = half * hd
    scale = hd ** -0.5 * LOG2E

    i = lax.axis_index("cx")
    j = lax.axis_index("cy")
    xx = j // 2
    c = lax.rem(j, 2)
    e = i * row_chips + xx
    par = lax.rem(e, 2)

    def dev(chip, core):
        return {"cx": chip // row_chips, "cy": lax.rem(chip, row_chips) * 2 + core}

    my_rows = pl.ds(pl.multiple_of(c * rows, rows), rows)
    x_in = pltpu.make_async_copy(x_ref, xv.at[my_rows], x_sem)
    x_in.start()

    def w_copy(s, t):
        col = pl.multiple_of((t * heads + s * chips) * hd + c * span, 128)
        return pltpu.make_async_copy(w_ref.at[:, pl.ds(col, span)], wv.at[3 * s + t], w_sem.at[3 * s + t])

    def wo_copy(s):
        part = pl.ds(s * chips * hd, chips * hd)
        return pltpu.make_async_copy(wo_ref.at[part], wov.at[part], wo_sem.at[s])

    for t in range(3):
        w_copy(0, t).start()

    n_dev = n_cx * n_cy
    barrier = pltpu.get_barrier_semaphore()

    def greet(k, _):
        other = lax.rem(i * n_cy + j + k, n_dev)
        pl.semaphore_signal(barrier, inc=1, device_id={"cx": other // n_cy, "cy": lax.rem(other, n_cy)},
                            device_id_type=MESH)
        return 0

    lax.fori_loop(1, n_dev, greet, 0)
    pl.semaphore_wait(barrier, n_dev - 1)

    x_in.wait()
    x_swap = pltpu.make_async_remote_copy(xv.at[my_rows], xv.at[my_rows], xs_sem, xr_sem,
                                          device_id=dev(e, 1 - c), device_id_type=MESH)
    x_swap.start()
    x_swap.wait()

    lane = lax.broadcasted_iota(jnp.int32, (kv_rows, 128), 1)
    low = lane < hd
    low_q = low[:rows]
    low_o = low[:rows // 2]

    def qkv_send(s, k):
        d = c * half + k
        return pltpu.make_async_remote_copy(stage.at[s, k], buf.at[s, e], qs_sem.at[s, k], qr_sem.at[s, e // 2],
                                            device_id=dev(d, par), device_id_type=MESH)

    def project(s):
        parts = []
        for t in range(3):
            w_copy(s, t).wait()
            if s + 1 < chunks:
                w_copy(s + 1, t).start()
            else:
                wo_copy(t).start()
            parts.append(jnp.dot(xv[...], wv[3 * s + t], preferred_element_type=F32))
        for p in range(half // 2):
            sl = slice(128 * p, 128 * p + 128)
            q, k, v = (a[:, sl] for a in parts)
            q_lo, q_hi = q[:rows], q[rows:]
            stage[s, 2 * p, 0:rows] = jnp.where(low_q, q_lo, pltpu.roll(q_hi, hd, 1)).astype(BF16)
            stage[s, 2 * p + 1, 0:rows] = jnp.where(low_q, pltpu.roll(q_lo, hd, 1), q_hi).astype(BF16)
            stage[s, 2 * p, rows:] = jnp.where(low, k, pltpu.roll(v, hd, 1)).astype(BF16)
            stage[s, 2 * p + 1, rows:] = jnp.where(low, pltpu.roll(k, hd, 1), v).astype(BF16)

        def send(n, _):
            dx = lax.rem(n // 2 + 1 + xx, row_chips)
            k = lax.rem(n, 2) * row_chips + dx
            mine = jnp.logical_and(c * half + k == e, par == c)

            @pl.when(mine)
            def _():
                buf[s, e] = stage[s, k]

            @pl.when(jnp.logical_not(mine))
            def _():
                qkv_send(s, k).start()
            return 0

        lax.fori_loop(0, half, send, 0)

    def sent(s):
        def one(k, _):
            @pl.when(jnp.logical_not(jnp.logical_and(c * half + k == e, par == c)))
            def _():
                qkv_send(s, k).wait_send()
            return 0

        lax.fori_loop(0, half, one, 0)

    def fwd(s, n, core):
        part = buf.at[s, 2 * n + core, pl.ds(rows, kv_rows)]
        return pltpu.make_async_remote_copy(part, part, fs_sem.at[s, n], fr_sem.at[s, n],
                                            device_id=dev(e, 1 - c), device_id_type=MESH)

    def forward(s):
        def one(n, _):
            src = 2 * n + c
            local = jnp.logical_and(src == e, e // half == c)

            @pl.when(jnp.logical_not(local))
            def _():
                pltpu.make_async_remote_copy(buf.at[s, src], buf.at[s, src], qs_sem.at[s, 0], qr_sem.at[s, n],
                                             device_id=dev(e, 1 - c), device_id_type=MESH).wait_recv()
            fwd(s, n, c).start()
            return 0

        lax.fori_loop(0, half, one, 0)

    def o_send(s, n, core):
        q_chip = 2 * n + c
        return pltpu.make_async_remote_copy(ostage.at[s, 2 * n + core], obuf.at[s, e], os_sem.at[s, 2 * n + core],
                                            or_sem.at[s, e], device_id=dev(q_chip, core), device_id_type=MESH)

    def attend(s):
        def got(n, _):
            fwd(s, n, 1 - c).wait_recv()
            return 0

        lax.fori_loop(0, half, got, 0)

        def block(b, _):
            qs = []
            for u in range(2):
                qq = buf[s, 2 * (2 * b + u) + c, 0:rows].astype(F32)
                qs.append(jnp.where(low_q, qq, 0.0).astype(BF16))
                qs.append(jnp.where(low_q, pltpu.roll(qq, hd, 1), 0.0).astype(BF16))
            q = jnp.concatenate(qs, axis=0)
            kv = jnp.concatenate([buf[s, n, rows:] for n in range(chips)], axis=0)
            logits = lax.dot_general(q, kv, (((1,), (1,)), ((), ())), preferred_element_type=F32)
            m = jnp.max(logits, axis=1, keepdims=True)
            w = jnp.exp2((logits - m) * scale)
            den = jnp.sum(w, axis=1, keepdims=True)
            o = jnp.dot(w.astype(BF16), kv, preferred_element_type=F32) / den
            hr = rows // 2
            for u in range(4):
                top, bot = o[u * rows:u * rows + hr], o[u * rows + hr:(u + 1) * rows]
                ostage[s, 4 * b + u] = jnp.where(low_o, pltpu.roll(top, hd, 1), bot).astype(BF16)
            for u in range(4):
                n, core = 2 * b + u // 2, u % 2
                mine = jnp.logical_and(2 * n + c == e, c == core)

                @pl.when(mine)
                def _():
                    obuf[s, e] = ostage[s, 4 * b + u]

                @pl.when(jnp.logical_not(mine))
                def _():
                    o_send(s, n, core).start()
            return 0

        lax.fori_loop(0, half // 2, block, 0)

    def o_sent(s):
        def one(n, _):
            for core in range(2):
                @pl.when(jnp.logical_not(jnp.logical_and(2 * n + c == e, c == core)))
                def _():
                    o_send(s, n, core).wait_send()
            return 0

        lax.fori_loop(0, half, one, 0)

    def output(s):
        def got(d, _):
            @pl.when(jnp.logical_not(jnp.logical_and(d == e, par == c)))
            def _():
                pltpu.make_async_remote_copy(obuf.at[s, d], obuf.at[s, d], os_sem.at[s, 0], or_sem.at[s, d],
                                             device_id=dev(e, 1 - c), device_id_type=MESH).wait_recv()
            return 0

        lax.fori_loop(0, chips, got, 0)
        wo_copy(s).wait()
        tiles = []
        for p in range(half):
            a, b = obuf[s, 2 * p].astype(F32), obuf[s, 2 * p + 1].astype(F32)
            top = jnp.where(low_o, a, pltpu.roll(b, hd, 1))
            bot = jnp.where(low_o, pltpu.roll(a, hd, 1), b)
            tiles.append(jnp.concatenate([top, bot], axis=0).astype(BF16))
        o = jnp.concatenate(tiles, axis=1)
        part = jnp.dot(o, wov[s * chips * hd:(s + 1) * chips * hd], preferred_element_type=F32)
        if s == 0:
            acc[...] = part
        elif s < chunks - 1:
            acc[...] += part
        else:
            y_ref[...] = (acc[...] + part).astype(BF16)

    for s in range(chunks):
        project(s)
    forward(0)
    attend(0)
    forward(1)
    attend(1)
    forward(2)
    output(0)
    attend(2)
    output(1)
    output(2)
    for s in range(chunks):
        sent(s)
        o_sent(s)

        def one(n, _):
            fwd(s, n, c).wait_send()
            return 0

        lax.fori_loop(0, half, one, 0)


def solution(mesh):
    n_cx, n_cy = mesh.shape["cx"], mesh.shape["cy"]
    chips = n_cx * n_cy // 2

    def attend_local(x_blk, w_qkv, w_o):
        heads, hd, width = w_o.shape
        rows = x_blk.shape[1]
        chunks = heads // chips
        half = chips // 2
        dma, vm = pltpu.SemaphoreType.DMA, pltpu.VMEM
        any_ = pl.BlockSpec(memory_space=pl.ANY)
        y = pl.pallas_call(
            functools.partial(kernel, (n_cx, n_cy, chips, chunks, heads, hd)),
            out_shape=jax.ShapeDtypeStruct((rows, width), BF16),
            in_specs=[any_, any_, any_],
            out_specs=pl.BlockSpec(memory_space=pltpu.VMEM),
            scratch_shapes=[
                vm((2 * rows, width), BF16),
                vm((3 * chunks, width, half * hd), BF16),
                vm((heads * hd, width), BF16),
                vm((chunks, half, 3 * rows, 128), BF16),
                vm((chunks, chips, 3 * rows, 128), BF16),
                vm((chunks, chips, rows // 2, 128), BF16),
                vm((chunks, chips, rows // 2, 128), BF16),
                vm((rows, width), F32),
                dma, dma((3 * chunks,)), dma((chunks,)), dma, dma,
                dma((chunks, half)), dma((chunks, half)),
                dma((chunks, half)), dma((chunks, half)),
                dma((chunks, chips)), dma((chunks, chips)),
            ],
            compiler_params=pltpu.CompilerParams(
                collective_id=0, has_side_effects=True, vmem_limit_bytes=63 * 2 ** 20),
        )(x_blk[0], w_qkv, w_o.reshape(heads * hd, width))
        return y[None]

    return jax.shard_map(
        attend_local, mesh=mesh,
        in_specs=(P("dp", ("cx", "cy"), None), P(None, None), P(None, None, None)),
        out_specs=P("dp", ("cx", "cy"), None), check_vma=False)
```

```python
import functools

import jax
import jax.numpy as jnp
from jax import lax
from jax.experimental import pallas as pl
from jax.experimental.pallas import tpu as pltpu
from jax.sharding import PartitionSpec as P

MESH = pl.DeviceIdType.MESH
BF16, F32 = jnp.bfloat16, jnp.float32
LOG2E = 1.4426950408889634
GROUPS = 2
BLOCKS = 2


def both(a, b):
    return jnp.logical_and(a, b)


def kernel(cfg, x_ref, w_ref, wo_ref, y_ref, xv, wv, stage, buf, ostage, obuf, acc,
           x_sem, w_sem, wo_sem, xs_sem, xr_sem, qs_sem, qr_sem, fs_sem, fr_sem, os_sem, or_sem):
    n_cx, n_cy, chips, chunks, heads, hd = cfg
    row_chips = n_cy // 2
    half = chips // 2
    rows, width = x_ref.shape
    kv_rows = 2 * rows
    span = half * hd
    scale = hd ** -0.5 * LOG2E
    group = half // GROUPS
    steps = chunks * GROUPS
    o_rows = chips * hd
    o_cols = group * hd
    o_parts = width // o_cols
    per = width // o_rows

    i = lax.axis_index("cx")
    j = lax.axis_index("cy")
    xx = lax.div(j, 2)
    c = lax.rem(j, 2)
    e = i * row_chips + xx
    par = lax.rem(e, 2)
    pair = lax.div(e, 2)

    def dev(chip, core):
        return {"cx": lax.div(chip, row_chips), "cy": lax.rem(chip, row_chips) * 2 + core}

    my_rows = pl.ds(pl.multiple_of(c * rows, rows), rows)
    x_in = pltpu.make_async_copy(x_ref, xv.at[my_rows], x_sem)
    x_in.start()

    def step(n):
        return lax.div(n, GROUPS), c * half + lax.rem(lax.rem(n, GROUPS) + i, GROUPS) * group

    def w_copy(n, t):
        s, first = step(n)
        col = pl.multiple_of((t * heads + s * chips + first) * hd, 128)
        return pltpu.make_async_copy(w_ref.at[:, pl.ds(col, group * hd)], wv.at[3 * n + t], w_sem.at[n])

    def wo_part(s, n):
        m = s * o_parts + n
        return wv.at[lax.div(m, per), pl.ds(pl.multiple_of(lax.rem(m, per) * o_rows, o_rows), o_rows)]

    def wo_copy(s, n):
        src = wo_ref.at[pl.ds(pl.multiple_of(s * o_rows, o_rows), o_rows), pl.ds(n * o_cols, o_cols)]
        return pltpu.make_async_copy(src, wo_part(s, n), wo_sem.at[s])

    def arrived(ref, sem):
        pltpu.make_async_copy(ref, ref, sem).wait()

    for t in range(3):
        w_copy(0, t).start()

    n_dev = n_cx * n_cy
    barrier = pltpu.get_barrier_semaphore()

    def greet(k, _):
        other = lax.rem(i * n_cy + j + k, n_dev)
        pl.semaphore_signal(barrier, inc=1, device_id={"cx": lax.div(other, n_cy), "cy": lax.rem(other, n_cy)},
                            device_id_type=MESH)
        return 0

    lax.fori_loop(1, n_dev, greet, 0)
    for t in range(3):
        w_copy(1, t).start()
    pl.semaphore_wait(barrier, n_dev - 1)

    x_in.wait()
    for t in range(3):
        w_copy(2, t).start()
    x_swap = pltpu.make_async_remote_copy(xv.at[my_rows], xv.at[my_rows], xs_sem, xr_sem,
                                          device_id=dev(e, 1 - c), device_id_type=MESH)
    x_swap.start()
    x_swap.wait()

    low = lax.broadcasted_iota(jnp.int32, (kv_rows, 128), 1) < hd
    low_q = low[:rows]
    low_o = low[:rows // 2]

    def qkv_send(n, kk):
        s, first = step(n)
        return pltpu.make_async_remote_copy(stage.at[s, slot(n) + kk], buf.at[s, par, pair], qs_sem.at[s], qr_sem.at[s],
                                            device_id=dev(first + kk, par), device_id_type=MESH)

    def slot(n):
        return lax.rem(n, GROUPS) * group

    def keeps(n, kk):
        return both(step(n)[1] + kk == e, par == c)

    def project(n):
        arrived(wv.at[pl.ds(3 * n, 3)], w_sem.at[n])

        @pl.when(n + 3 < steps)
        def _():
            for t in range(3):
                w_copy(n + 3, t).start()

        q, k, v = (jnp.dot(xv[...], wv[3 * n + t], preferred_element_type=F32) for t in range(3))
        s, at = lax.div(n, GROUPS), slot(n)
        for p in range(group // 2):
            sl = slice(128 * p, 128 * p + 128)
            q_lo, q_hi = q[:rows, sl], q[rows:, sl]
            stage[s, at + 2 * p, 0:rows] = jnp.where(low_q, q_lo, pltpu.roll(q_hi, hd, 1)).astype(BF16)
            stage[s, at + 2 * p + 1, 0:rows] = jnp.where(low_q, pltpu.roll(q_lo, hd, 1), q_hi).astype(BF16)
            stage[s, at + 2 * p, rows:] = jnp.where(low, k[:, sl], pltpu.roll(v[:, sl], hd, 1)).astype(BF16)
            stage[s, at + 2 * p + 1, rows:] = jnp.where(low, pltpu.roll(k[:, sl], hd, 1), v[:, sl]).astype(BF16)
        for m in range(1, group):
            qkv_send(n, lax.rem(xx + m, group)).start()
        own = lax.rem(xx, group)

        @pl.when(keeps(n, own))
        def _():
            buf[s, par, pair] = stage[s, at + own]

        @pl.when(jnp.logical_not(keeps(n, own)))
        def _():
            qkv_send(n, own).start()

    local = both(lax.div(e, half) == c, par == c)

    def of(ref, count, less):
        def wait(sem):
            @pl.when(less)
            def _():
                arrived(ref.at[pl.ds(0, count - 1)], sem)

            @pl.when(jnp.logical_not(less))
            def _():
                arrived(ref, sem)
        return wait

    def fwd(s, core):
        part = buf.at[s, core, :, pl.ds(rows, kv_rows)]
        return pltpu.make_async_remote_copy(part, part, fs_sem.at[s], fr_sem.at[s],
                                            device_id=dev(e, 1 - c), device_id_type=MESH)

    def forward(s):
        of(buf.at[s, c], half, local)(qr_sem.at[s])
        fwd(s, c).start()

    def o_send(s, u):
        return pltpu.make_async_remote_copy(ostage.at[s, u], obuf.at[s, e], os_sem.at[s], or_sem.at[s],
                                            device_id=dev(2 * lax.div(u, 2) + c, lax.rem(u, 2)), device_id_type=MESH)

    own_u = 2 * pair + c
    part_u = chips // BLOCKS

    def attend(s, b):
        qs = []
        for n in range(half // BLOCKS):
            qq = buf[s, c, b * (half // BLOCKS) + n, 0:rows].astype(F32)
            qs.append(jnp.where(low_q, qq, 0.0).astype(BF16))
            qs.append(jnp.where(low_q, pltpu.roll(qq, hd, 1), 0.0).astype(BF16))
        q = jnp.concatenate(qs, axis=0)
        m = den = o = None
        for side in range(2):
            kv = jnp.concatenate([buf[s, side, n, rows:] for n in range(half)], axis=0)
            logits = lax.dot_general(q, kv, (((1,), (1,)), ((), ())), preferred_element_type=F32)
            top = jnp.max(logits, axis=1, keepdims=True)
            new = top if side == 0 else jnp.maximum(m, top)
            w = jnp.exp2((logits - new) * scale)
            part = jnp.sum(w, axis=1, keepdims=True)
            wkv = jnp.dot(w.astype(BF16), kv, preferred_element_type=F32)
            if side == 0:
                m, den, o = new, part, wkv
            else:
                old = jnp.exp2((m - new) * scale)
                den = den * old + part
                o = (o * old + wkv) / den
        hr = rows // 2
        for u in range(part_u):
            lo, hi = o[u * rows:u * rows + hr], o[u * rows + hr:(u + 1) * rows]
            ostage[s, b * part_u + u] = jnp.where(low_o, pltpu.roll(lo, hd, 1), hi).astype(BF16)
        first = b * part_u + lax.rem(own_u, part_u)
        stays = both(first == own_u, par == c)
        for k in range(1, part_u):
            o_send(s, b * part_u + lax.rem(own_u + k, part_u)).start()

        @pl.when(stays)
        def _():
            obuf[s, e] = ostage[s, own_u]

        @pl.when(jnp.logical_not(stays))
        def _():
            o_send(s, first).start()

    def output(s):
        of(obuf.at[s], chips, par == c)(or_sem.at[s])
        tiles = []
        for p in range(half):
            a, b = obuf[s, 2 * p].astype(F32), obuf[s, 2 * p + 1].astype(F32)
            top = jnp.where(low_o, a, pltpu.roll(b, hd, 1))
            bot = jnp.where(low_o, pltpu.roll(a, hd, 1), b)
            tiles.append(jnp.concatenate([top, bot], axis=0).astype(BF16))
        o = jnp.concatenate(tiles, axis=1)
        arrived(wv.at[pl.ds(s * (o_parts // per), o_parts // per)], wo_sem.at[s])
        for n in range(o_parts):
            acc[:, n * o_cols:(n + 1) * o_cols] += jnp.dot(o, wo_part(s, n)[...], preferred_element_type=F32)

    def project_loop(n, _):
        project(n)
        return 0

    lax.fori_loop(0, steps, project_loop, 0)
    for s in range(chunks):
        for n in range(o_parts):
            wo_copy(s, n).start()
    acc[...] = jnp.zeros_like(acc)

    forward(0)

    def block_loop(n, _):
        s, b = lax.div(n, BLOCKS), lax.rem(n, BLOCKS)

        @pl.when(b == 0)
        def _():
            fwd(s, 1 - c).wait_recv()

        attend(s, b)

        @pl.when(both(b == 0, s + 1 < chunks))
        def _():
            forward(s + 1)

        @pl.when(both(b == BLOCKS - 1, s > 0))
        def _():
            output(s - 1)
        return 0

    lax.fori_loop(0, chunks * BLOCKS, block_loop, 0)
    output(chunks - 1)
    y_ref[...] = acc[...].astype(BF16)

    for s in range(chunks):
        of(stage.at[s], half, local)(qs_sem.at[s])
        fwd(s, c).wait_send()
        of(ostage.at[s], chips, par == c)(os_sem.at[s])


def solution(mesh):
    n_cx, n_cy = mesh.shape["cx"], mesh.shape["cy"]
    chips = n_cx * n_cy // 2

    def attend_local(x_blk, w_qkv, w_o):
        heads, hd, width = w_o.shape
        rows = x_blk.shape[1]
        chunks = heads // chips
        half = chips // 2
        group = half // GROUPS
        steps = chunks * GROUPS
        dma, vm = pltpu.SemaphoreType.DMA, pltpu.VMEM
        y = pl.pallas_call(
            functools.partial(kernel, (n_cx, n_cy, chips, chunks, heads, hd)),
            out_shape=pltpu.VMEM((rows, width), BF16),
            in_specs=[pl.BlockSpec(memory_space=pltpu.HBM)] * 3,
            out_specs=pl.BlockSpec(memory_space=pltpu.VMEM),
            scratch_shapes=[
                vm((2 * rows, width), BF16),
                vm((3 * steps, width, group * hd), BF16),
                vm((chunks, half, 3 * rows, 128), BF16),
                vm((chunks, 2, half, 3 * rows, 128), BF16),
                vm((chunks, chips, rows // 2, 128), BF16),
                vm((chunks, chips, rows // 2, 128), BF16),
                vm((rows, width), F32),
                dma, dma((steps,)), dma((chunks,)), dma, dma,
                dma((chunks,)), dma((chunks,)), dma((chunks,)), dma((chunks,)), dma((chunks,)), dma((chunks,)),
            ],
            compiler_params=pltpu.CompilerParams(
                collective_id=0, has_side_effects=True, vmem_limit_bytes=56 * 2 ** 20),
        )(x_blk[0], w_qkv, w_o.reshape(heads * hd, width))
        return y[None]

    return jax.shard_map(
        attend_local, mesh=mesh,
        in_specs=(P("dp", ("cx", "cy"), None), P(None, None), P(None, None, None)),
        out_specs=P("dp", ("cx", "cy"), None), check_vma=False)
```

```python
import functools

import jax
import jax.numpy as jnp
from jax import lax
from jax.experimental import pallas as pl
from jax.experimental.pallas import tpu as pltpu
from jax.sharding import PartitionSpec as P

MESH = pl.DeviceIdType.MESH
BF16, F32 = jnp.bfloat16, jnp.float32
LOG2E = 1.4426950408889634
GROUPS = 2
KEY_PARTS = 2
ORDER = (1, 3, 2)


def both(a, b):
    return jnp.logical_and(a, b)


def kernel(cfg, x_ref, w_ref, wo_ref, y_ref, xv, wv, stage, buf, ostage, obuf, acc,
           x_sem, w_sem, wo_sem, xs_sem, xr_sem, qs_sem, qr_sem, fs_sem, fr_sem, os_sem, or_sem):
    n_cx, n_cy, chips, chunks, heads, hd = cfg
    row_chips = n_cy // 2
    half = chips // 2
    rows, width = x_ref.shape
    kv_rows = 2 * rows
    span = half * hd
    scale = hd ** -0.5 * LOG2E
    group = half // GROUPS
    steps = chunks * GROUPS
    o_rows = chips * hd
    o_cols = group * hd
    o_parts = width // o_cols
    per = width // o_rows

    i = lax.axis_index("cx")
    j = lax.axis_index("cy")
    xx = lax.div(j, 2)
    c = lax.rem(j, 2)
    e = i * row_chips + xx
    par = lax.rem(e, 2)
    pair = lax.div(e, 2)

    def dev(chip, core):
        return {"cx": lax.div(chip, row_chips), "cy": lax.rem(chip, row_chips) * 2 + core}

    my_rows = pl.ds(pl.multiple_of(c * rows, rows), rows)
    x_in = pltpu.make_async_copy(x_ref, xv.at[my_rows], x_sem)
    x_in.start()

    def step(n):
        return lax.div(n, GROUPS), c * half + lax.rem(lax.rem(n, GROUPS) + i, GROUPS) * group

    def w_copy(n, t):
        s, first = step(n)
        col = pl.multiple_of((t * heads + s * chips + first) * hd, 128)
        return pltpu.make_async_copy(w_ref.at[:, pl.ds(col, group * hd)], wv.at[3 * n + t], w_sem.at[n])

    def wo_part(s, n):
        m = s * o_parts + n
        return wv.at[lax.div(m, per), pl.ds(pl.multiple_of(lax.rem(m, per) * o_rows, o_rows), o_rows)]

    def wo_copy(s, n):
        src = wo_ref.at[pl.ds(pl.multiple_of(s * o_rows, o_rows), o_rows), pl.ds(n * o_cols, o_cols)]
        return pltpu.make_async_copy(src, wo_part(s, n), wo_sem.at[s])

    def arrived(ref, sem):
        pltpu.make_async_copy(ref, ref, sem).wait()

    n_dev = n_cx * n_cy
    barrier = pltpu.get_barrier_semaphore()

    def greet(k, _):
        other = lax.rem(i * n_cy + j + k, n_dev)
        pl.semaphore_signal(barrier, inc=1, device_id={"cx": lax.div(other, n_cy), "cy": lax.rem(other, n_cy)},
                            device_id_type=MESH)
        return 0

    lax.fori_loop(1, n_dev // 2, greet, 0)
    for t in range(3):
        w_copy(0, t).start()
    lax.fori_loop(n_dev // 2, n_dev, greet, 0)
    for t in range(3):
        w_copy(1, t).start()
    pl.semaphore_wait(barrier, n_dev - 1)

    x_in.wait()
    for t in range(3):
        w_copy(2, t).start()
    x_swap = pltpu.make_async_remote_copy(xv.at[my_rows], xv.at[my_rows], xs_sem, xr_sem,
                                          device_id=dev(e, 1 - c), device_id_type=MESH)
    x_swap.start()
    x_swap.wait()

    low = lax.broadcasted_iota(jnp.int32, (kv_rows, 128), 1) < hd
    low_q = low[:rows]
    low_o = low[:rows // 2]

    def qkv_send(n, kk):
        s, first = step(n)
        return pltpu.make_async_remote_copy(stage.at[s, slot(n) + kk], buf.at[s, par, pair], qs_sem.at[s], qr_sem.at[s],
                                            device_id=dev(first + kk, par), device_id_type=MESH)

    def slot(n):
        return lax.rem(n, GROUPS) * group

    def keeps(n, kk):
        return both(step(n)[1] + kk == e, par == c)

    def project(n):
        arrived(wv.at[pl.ds(3 * n, 3)], w_sem.at[n])

        @pl.when(n + 3 < steps)
        def _():
            for t in range(3):
                w_copy(n + 3, t).start()

        q, k, v = (jnp.dot(xv[...], wv[3 * n + t], preferred_element_type=F32) for t in range(3))
        s, at = lax.div(n, GROUPS), slot(n)
        for p in range(group // 2):
            sl = slice(128 * p, 128 * p + 128)
            q_lo, q_hi = q[:rows, sl], q[rows:, sl]
            stage[s, at + 2 * p, 0:rows] = jnp.where(low_q, q_lo, pltpu.roll(q_hi, hd, 1)).astype(BF16)
            stage[s, at + 2 * p + 1, 0:rows] = jnp.where(low_q, pltpu.roll(q_lo, hd, 1), q_hi).astype(BF16)
            stage[s, at + 2 * p, rows:] = jnp.where(low, k[:, sl], pltpu.roll(v[:, sl], hd, 1)).astype(BF16)
            stage[s, at + 2 * p + 1, rows:] = jnp.where(low, pltpu.roll(k[:, sl], hd, 1), v[:, sl]).astype(BF16)
        for m in ORDER:
            qkv_send(n, lax.rem(xx + m, group)).start()
        own = lax.rem(xx, group)

        @pl.when(keeps(n, own))
        def _():
            buf[s, par, pair] = stage[s, at + own]

        @pl.when(jnp.logical_not(keeps(n, own)))
        def _():
            qkv_send(n, own).start()

    local = both(lax.div(e, half) == c, par == c)

    def of(ref, count, less):
        def wait(sem):
            @pl.when(less)
            def _():
                arrived(ref.at[pl.ds(0, count - 1)], sem)

            @pl.when(jnp.logical_not(less))
            def _():
                arrived(ref, sem)
        return wait

    def fwd(s, core):
        part = buf.at[s, core, :, pl.ds(rows, kv_rows)]
        return pltpu.make_async_remote_copy(part, part, fs_sem.at[s], fr_sem.at[s],
                                            device_id=dev(e, 1 - c), device_id_type=MESH)

    def forward(s):
        of(buf.at[s, c], half, local)(qr_sem.at[s])
        fwd(s, c).start()

    def o_send(s, u):
        return pltpu.make_async_remote_copy(ostage.at[s, u], obuf.at[s, e], os_sem.at[s], or_sem.at[s],
                                            device_id=dev(2 * lax.div(u, 2) + c, lax.rem(u, 2)), device_id_type=MESH)

    own_u = 2 * pair + c
    key_chips = half // KEY_PARTS

    def attend(s):
        qs = []
        for n in range(half):
            qq = buf[s, c, n, 0:rows].astype(F32)
            qs.append(jnp.where(low_q, qq, 0.0).astype(BF16))
            qs.append(jnp.where(low_q, pltpu.roll(qq, hd, 1), 0.0).astype(BF16))
        q = jnp.concatenate(qs, axis=0)
        m = den = o = None
        for side in range(2):
            core = c if side == 0 else 1 - c
            if side == 1:
                fwd(s, 1 - c).wait_recv()
            for g in range(KEY_PARTS):
                kv = jnp.concatenate([buf[s, core, g * key_chips + n, rows:] for n in range(key_chips)], axis=0)
                logits = lax.dot_general(q, kv, (((1,), (1,)), ((), ())), preferred_element_type=F32)
                top = jnp.max(logits, axis=1, keepdims=True)
                new = top if m is None else jnp.maximum(m, top)
                w = jnp.exp2((logits - new) * scale)
                part = jnp.sum(w, axis=1, keepdims=True)
                wkv = jnp.dot(w.astype(BF16), kv, preferred_element_type=F32)
                if m is None:
                    den, o = part, wkv
                else:
                    old = jnp.exp2((m - new) * scale)
                    den, o = den * old + part, o * old + wkv
                m = new
        o = o / den
        hr = rows // 2
        for u in range(chips):
            lo, hi = o[u * rows:u * rows + hr], o[u * rows + hr:(u + 1) * rows]
            ostage[s, u] = jnp.where(low_o, pltpu.roll(lo, hd, 1), hi).astype(BF16)

        for k in range(1, chips):
            o_send(s, lax.rem(own_u + k, chips)).start()

        @pl.when(par == c)
        def _():
            obuf[s, e] = ostage[s, own_u]

        @pl.when(par != c)
        def _():
            o_send(s, own_u).start()

    def output(s, last=False):
        of(obuf.at[s], chips, par == c)(or_sem.at[s])
        tiles = []
        for p in range(half):
            a, b = obuf[s, 2 * p].astype(F32), obuf[s, 2 * p + 1].astype(F32)
            top = jnp.where(low_o, a, pltpu.roll(b, hd, 1))
            bot = jnp.where(low_o, pltpu.roll(a, hd, 1), b)
            tiles.append(jnp.concatenate([top, bot], axis=0).astype(BF16))
        o = jnp.concatenate(tiles, axis=1)
        arrived(wv.at[pl.ds(s * (o_parts // per), o_parts // per)], wo_sem.at[s])
        for n in range(o_parts):
            cols = slice(n * o_cols, (n + 1) * o_cols)
            total = acc[:, cols] + jnp.dot(o, wo_part(s, n)[...], preferred_element_type=F32)
            if last:
                y_ref[:, cols] = total.astype(BF16)
            else:
                acc[:, cols] = total

    def project_loop(n, _):
        project(n)
        return 0

    lax.fori_loop(0, steps, project_loop, 0)
    for s in range(chunks):
        for n in range(o_parts):
            wo_copy(s, n).start()
    acc[...] = jnp.zeros_like(acc)

    def chunk_loop(s, _):
        forward(s)
        attend(s)
        return 0

    lax.fori_loop(0, chunks, chunk_loop, 0)
    for s in range(chunks - 1):
        output(s)
    output(chunks - 1, last=True)

    for s in range(chunks):
        of(stage.at[s], half, local)(qs_sem.at[s])
        fwd(s, c).wait_send()
        of(ostage.at[s], chips, par == c)(os_sem.at[s])


def solution(mesh):
    n_cx, n_cy = mesh.shape["cx"], mesh.shape["cy"]
    chips = n_cx * n_cy // 2

    def attend_local(x_blk, w_qkv, w_o):
        heads, hd, width = w_o.shape
        rows = x_blk.shape[1]
        chunks = heads // chips
        half = chips // 2
        group = half // GROUPS
        steps = chunks * GROUPS
        dma, vm = pltpu.SemaphoreType.DMA, pltpu.VMEM
        y = pl.pallas_call(
            functools.partial(kernel, (n_cx, n_cy, chips, chunks, heads, hd)),
            out_shape=pltpu.VMEM((rows, width), BF16),
            in_specs=[pl.BlockSpec(memory_space=pltpu.HBM)] * 3,
            out_specs=pl.BlockSpec(memory_space=pltpu.VMEM),
            scratch_shapes=[
                vm((2 * rows, width), BF16),
                vm((3 * steps, width, group * hd), BF16),
                vm((chunks, half, 3 * rows, 128), BF16),
                vm((chunks, 2, half, 3 * rows, 128), BF16),
                vm((chunks, chips, rows // 2, 128), BF16),
                vm((chunks, chips, rows // 2, 128), BF16),
                vm((rows, width), F32),
                dma, dma((steps,)), dma((chunks,)), dma, dma,
                dma((chunks,)), dma((chunks,)), dma((chunks,)), dma((chunks,)), dma((chunks,)), dma((chunks,)),
            ],
            compiler_params=pltpu.CompilerParams(
                collective_id=0, has_side_effects=True, vmem_limit_bytes=56 * 2 ** 20),
        )(x_blk[0], w_qkv, w_o.reshape(heads * hd, width))
        return y[None]

    return jax.shard_map(
        attend_local, mesh=mesh,
        in_specs=(P("dp", ("cx", "cy"), None), P(None, None), P(None, None, None)),
        out_specs=P("dp", ("cx", "cy"), None), check_vma=False)
```

```python
import functools

import jax
import jax.numpy as jnp
from jax import lax
from jax.experimental import pallas as pl
from jax.experimental.pallas import tpu as pltpu
from jax.sharding import PartitionSpec as P

MESH = pl.DeviceIdType.MESH
BF16, F32 = jnp.bfloat16, jnp.float32
LOG2E = 1.4426950408889634
GROUPS = 2
KEY_PARTS = 2
ORDER = (1, 3, 2)


def both(a, b):
    return jnp.logical_and(a, b)


def kernel(cfg, x_ref, w_ref, wo_ref, y_ref, xv, wv, stage, buf, ostage, obuf, acc,
           x_sem, w_sem, wo_sem, xs_sem, xr_sem, qs_sem, qr_sem, fs_sem, fr_sem, os_sem, or_sem):
    n_cx, n_cy, chips, chunks, heads, hd = cfg
    row_chips = n_cy // 2
    half = chips // 2
    rows, width = x_ref.shape
    span = half * hd
    scale = hd ** -0.5 * LOG2E
    group = half // GROUPS
    steps = chunks * GROUPS
    o_rows = chips * hd
    o_cols = group * hd
    o_parts = width // o_cols
    per = width // o_rows

    i = lax.axis_index("cx")
    j = lax.axis_index("cy")
    xx = lax.div(j, 2)
    c = lax.rem(j, 2)
    e = i * row_chips + xx
    par = lax.rem(e, 2)
    pair = lax.div(e, 2)

    def dev(chip, core):
        return {"cx": lax.div(chip, row_chips), "cy": lax.rem(chip, row_chips) * 2 + core}

    my_rows = pl.ds(pl.multiple_of(c * rows, rows), rows)
    x_in = pltpu.make_async_copy(x_ref, xv.at[my_rows], x_sem)
    x_in.start()

    def step(n):
        return lax.div(n, GROUPS), c * half + lax.rem(lax.rem(n, GROUPS) + i, GROUPS) * group

    def w_copy(n, t):
        s, first = step(n)
        col = pl.multiple_of((t * heads + s * chips + first) * hd, 128)
        return pltpu.make_async_copy(w_ref.at[:, pl.ds(col, group * hd)], wv.at[3 * n + t], w_sem.at[n])

    def wo_part(s, n):
        m = s * o_parts + n
        return wv.at[lax.div(m, per), pl.ds(pl.multiple_of(lax.rem(m, per) * o_rows, o_rows), o_rows)]

    def wo_copy(s, n):
        src = wo_ref.at[pl.ds(pl.multiple_of(s * o_rows, o_rows), o_rows), pl.ds(n * o_cols, o_cols)]
        return pltpu.make_async_copy(src, wo_part(s, n), wo_sem.at[s])

    def w_start(n):
        for t in range(3):
            w_copy(n, t).start()

    def arrived(ref, sem):
        pltpu.make_async_copy(ref, ref, sem).wait()

    n_dev = n_cx * n_cy
    barrier = pltpu.get_barrier_semaphore()

    def greet(k, _):
        other = lax.rem(i * n_cy + j + k, n_dev)
        pl.semaphore_signal(barrier, inc=1, device_id={"cx": lax.div(other, n_cy), "cy": lax.rem(other, n_cy)},
                            device_id_type=MESH)
        return 0

    lax.fori_loop(1, n_dev // 2, greet, 0)
    w_start(0)
    lax.fori_loop(n_dev // 2, n_dev, greet, 0)
    w_start(1)

    low = lax.broadcasted_iota(jnp.int32, (rows, 128), 1) < hd
    low_o = low[:rows // 2]
    q_rows = rows // 2

    def slot(n):
        return lax.rem(n, GROUPS) * group

    def keeps(n, kk):
        return both(step(n)[1] + kk == e, par == c)

    def qkv_send(n, kk, r=None):
        s, first = step(n)
        src, dst = stage.at[s, slot(n) + kk], buf.at[s, par, pair]
        if r is not None:
            src, dst = src.at[r], dst.at[r]
        return pltpu.make_async_remote_copy(src, dst, qs_sem.at[s], qr_sem.at[s],
                                            device_id=dev(first + kk, par), device_id_type=MESH)

    def send(n, r=None):
        for m in ORDER:
            qkv_send(n, lax.rem(xx + m, group), r).start()
        own = lax.rem(xx, group)
        s = lax.div(n, GROUPS)

        @pl.when(keeps(n, own))
        def _():
            if r is None:
                buf[s, par, pair] = stage[s, slot(n) + own]
            else:
                buf[s, par, pair, r] = stage[s, slot(n) + own, r]

        @pl.when(jnp.logical_not(keeps(n, own)))
        def _():
            qkv_send(n, own, r).start()

    def pack(n, r, q, k, v):
        s, at = lax.div(n, GROUPS), slot(n)
        for p in range(group // 2):
            sl = slice(128 * p, 128 * p + 128)
            top, bot, kk, vv = q[:q_rows, sl], q[q_rows:, sl], k[:, sl], v[:, sl]
            stage[s, at + 2 * p, r, 0:q_rows] = jnp.where(low_o, top, pltpu.roll(bot, hd, 1)).astype(BF16)
            stage[s, at + 2 * p + 1, r, 0:q_rows] = jnp.where(low_o, pltpu.roll(top, hd, 1), bot).astype(BF16)
            stage[s, at + 2 * p, r, q_rows:] = jnp.where(low, kk, pltpu.roll(vv, hd, 1)).astype(BF16)
            stage[s, at + 2 * p + 1, r, q_rows:] = jnp.where(low, pltpu.roll(kk, hd, 1), vv).astype(BF16)

    def project_half(n, r):
        x_half = xv[pl.ds(pl.multiple_of(r * rows, rows), rows)]
        pack(n, r, *(jnp.dot(x_half, wv[3 * n + t], preferred_element_type=F32) for t in range(3)))

    def project(n):
        arrived(wv.at[pl.ds(3 * n, 3)], w_sem.at[n])
        q, k, v = (jnp.dot(xv[...], wv[3 * n + t], preferred_element_type=F32) for t in range(3))
        for r in range(2):
            half_rows = slice(r * rows, (r + 1) * rows)
            pack(n, r, q[half_rows], k[half_rows], v[half_rows])
        send(n)

    x_in.wait()
    arrived(wv.at[pl.ds(0, 3)], w_sem.at[0])
    w_start(2)
    w_start(3)
    project_half(0, c)
    pl.semaphore_wait(barrier, n_dev - 1)
    x_swap = pltpu.make_async_remote_copy(xv.at[my_rows], xv.at[my_rows], xs_sem, xr_sem,
                                          device_id=dev(e, 1 - c), device_id_type=MESH)
    x_swap.start()
    send(0, c)
    for n in range(1, GROUPS):
        arrived(wv.at[pl.ds(3 * n, 3)], w_sem.at[n])
        for m in range(n + 3, min(steps, GROUPS + n + 3)):
            w_start(m)
        project_half(n, c)
        send(n, c)
    x_swap.wait()
    for n in range(GROUPS):
        project_half(n, 1 - c)
        send(n, 1 - c)

    local = both(lax.div(e, half) == c, par == c)

    def of(ref, count, less):
        def wait(sem):
            @pl.when(less)
            def _():
                arrived(ref.at[pl.ds(0, count - 1)], sem)

            @pl.when(jnp.logical_not(less))
            def _():
                arrived(ref, sem)
        return wait

    def fwd(s, core):
        part = buf.at[s, core, :, :, pl.ds(q_rows, rows)]
        return pltpu.make_async_remote_copy(part, part, fs_sem.at[s], fr_sem.at[s],
                                            device_id=dev(e, 1 - c), device_id_type=MESH)

    def forward(s):
        of(buf.at[s, c], half, local)(qr_sem.at[s])
        fwd(s, c).start()

    def o_send(s, u):
        return pltpu.make_async_remote_copy(ostage.at[s, u], obuf.at[s, e], os_sem.at[s], or_sem.at[s],
                                            device_id=dev(2 * lax.div(u, 2) + c, lax.rem(u, 2)), device_id_type=MESH)

    own_u = 2 * pair + c
    key_chips = half // KEY_PARTS

    def attend(s):
        qs = []
        for n in range(half):
            for r in range(2):
                qq = buf[s, c, n, r, 0:q_rows].astype(F32)
                qs.append(jnp.where(low_o, qq, 0.0).astype(BF16))
                qs.append(jnp.where(low_o, pltpu.roll(qq, hd, 1), 0.0).astype(BF16))
        q = jnp.concatenate(qs, axis=0)
        m = den = o = None
        for side in range(2):
            core = c if side == 0 else 1 - c
            if side == 1:
                fwd(s, 1 - c).wait_recv()
            for g in range(KEY_PARTS):
                kv = jnp.concatenate([buf[s, core, g * key_chips + n, r, q_rows:]
                                      for n in range(key_chips) for r in range(2)], axis=0)
                logits = lax.dot_general(q, kv, (((1,), (1,)), ((), ())), preferred_element_type=F32)
                top = jnp.max(logits, axis=1, keepdims=True)
                new = top if m is None else jnp.maximum(m, top)
                w = jnp.exp2((logits - new) * scale)
                part = jnp.sum(w, axis=1, keepdims=True)
                wkv = jnp.dot(w.astype(BF16), kv, preferred_element_type=F32)
                if m is None:
                    den, o = part, wkv
                else:
                    old = jnp.exp2((m - new) * scale)
                    den, o = den * old + part, o * old + wkv
                m = new
        o = o / den
        hr = rows // 2
        for u in range(chips):
            lo, hi = o[u * rows:u * rows + hr], o[u * rows + hr:(u + 1) * rows]
            ostage[s, u] = jnp.where(low_o, pltpu.roll(lo, hd, 1), hi).astype(BF16)

        for k in range(1, chips):
            o_send(s, lax.rem(own_u + k, chips)).start()

        @pl.when(par == c)
        def _():
            obuf[s, e] = ostage[s, own_u]

        @pl.when(par != c)
        def _():
            o_send(s, own_u).start()

    def output(s, last=False):
        of(obuf.at[s], chips, par == c)(or_sem.at[s])
        tiles = []
        for p in range(half):
            a, b = obuf[s, 2 * p].astype(F32), obuf[s, 2 * p + 1].astype(F32)
            top = jnp.where(low_o, a, pltpu.roll(b, hd, 1))
            bot = jnp.where(low_o, pltpu.roll(a, hd, 1), b)
            tiles.append(jnp.concatenate([top, bot], axis=0).astype(BF16))
        o = jnp.concatenate(tiles, axis=1)
        arrived(wv.at[pl.ds(s * (o_parts // per), o_parts // per)], wo_sem.at[s])
        for n in range(o_parts):
            cols = slice(n * o_cols, (n + 1) * o_cols)
            total = acc[:, cols] + jnp.dot(o, wo_part(s, n)[...], preferred_element_type=F32)
            if last:
                y_ref[:, cols] = total.astype(BF16)
            else:
                acc[:, cols] = total

    def project_loop(n, _):
        project(n)
        return 0

    lax.fori_loop(GROUPS, steps, project_loop, 0)
    for s in range(chunks):
        for n in range(o_parts):
            wo_copy(s, n).start()
    acc[...] = jnp.zeros_like(acc)

    def chunk_loop(s, _):
        forward(s)
        attend(s)
        return 0

    lax.fori_loop(0, chunks, chunk_loop, 0)
    for s in range(chunks - 1):
        output(s)
    output(chunks - 1, last=True)

    for s in range(chunks):
        of(stage.at[s], half, local)(qs_sem.at[s])
        fwd(s, c).wait_send()
        of(ostage.at[s], chips, par == c)(os_sem.at[s])


def solution(mesh):
    n_cx, n_cy = mesh.shape["cx"], mesh.shape["cy"]
    chips = n_cx * n_cy // 2

    def attend_local(x_blk, w_qkv, w_o):
        heads, hd, width = w_o.shape
        rows = x_blk.shape[1]
        chunks = heads // chips
        half = chips // 2
        group = half // GROUPS
        steps = chunks * GROUPS
        dma, vm = pltpu.SemaphoreType.DMA, pltpu.VMEM
        y = pl.pallas_call(
            functools.partial(kernel, (n_cx, n_cy, chips, chunks, heads, hd)),
            out_shape=pltpu.VMEM((rows, width), BF16),
            in_specs=[pl.BlockSpec(memory_space=pltpu.HBM)] * 3,
            out_specs=pl.BlockSpec(memory_space=pltpu.VMEM),
            scratch_shapes=[
                vm((2 * rows, width), BF16),
                vm((3 * steps, width, group * hd), BF16),
                vm((chunks, half, 2, 3 * rows // 2, 128), BF16),
                vm((chunks, 2, half, 2, 3 * rows // 2, 128), BF16),
                vm((chunks, chips, rows // 2, 128), BF16),
                vm((chunks, chips, rows // 2, 128), BF16),
                vm((rows, width), F32),
                dma, dma((steps,)), dma((chunks,)), dma, dma,
                dma((chunks,)), dma((chunks,)), dma((chunks,)), dma((chunks,)), dma((chunks,)), dma((chunks,)),
            ],
            compiler_params=pltpu.CompilerParams(
                collective_id=0, has_side_effects=True, vmem_limit_bytes=56 * 2 ** 20),
        )(x_blk[0], w_qkv, w_o.reshape(heads * hd, width))
        return y[None]

    return jax.shard_map(
        attend_local, mesh=mesh,
        in_specs=(P("dp", ("cx", "cy"), None), P(None, None), P(None, None, None)),
        out_specs=P("dp", ("cx", "cy"), None), check_vma=False)
```

```python
import functools

import jax
import jax.numpy as jnp
from jax import lax
from jax.experimental import pallas as pl
from jax.experimental.pallas import tpu as pltpu
from jax.sharding import PartitionSpec as P

MESH = pl.DeviceIdType.MESH
BF16, F32 = jnp.bfloat16, jnp.float32
LOG2E = 1.4426950408889634
GROUPS = 2
KEY_PARTS = 2
ORDER = (1, 3, 2)


def both(a, b):
    return jnp.logical_and(a, b)


def kernel(cfg, x_ref, w_ref, wo_ref, y_ref, xv, wv, stage, buf, ostage, obuf, acc,
           x_sem, w_sem, wo_sem, xs_sem, xr_sem, qs_sem, qr_sem, fs_sem, fr_sem, os_sem, or_sem):
    n_cx, n_cy, chips, chunks, heads, hd = cfg
    row_chips = n_cy // 2
    half = chips // 2
    rows, width = x_ref.shape
    span = half * hd
    scale = hd ** -0.5 * LOG2E
    group = half // GROUPS
    steps = chunks * GROUPS
    o_rows = chips * hd
    o_cols = group * hd
    o_parts = width // o_cols
    per = width // o_rows

    i = lax.axis_index("cx")
    j = lax.axis_index("cy")
    xx = lax.div(j, 2)
    c = lax.rem(j, 2)
    e = i * row_chips + xx
    par = lax.rem(e, 2)
    pair = lax.div(e, 2)

    def dev(chip, core):
        return {"cx": lax.div(chip, row_chips), "cy": lax.rem(chip, row_chips) * 2 + core}

    my_rows = pl.ds(pl.multiple_of(c * rows, rows), rows)
    x_in = pltpu.make_async_copy(x_ref, xv.at[my_rows], x_sem)
    x_in.start()

    def step(n):
        return lax.div(n, GROUPS), c * half + lax.rem(lax.rem(n, GROUPS) + i, GROUPS) * group

    def w_copy(n, t):
        s, first = step(n)
        col = pl.multiple_of((t * heads + s * chips + first) * hd, 128)
        return pltpu.make_async_copy(w_ref.at[:, pl.ds(col, group * hd)], wv.at[3 * n + t], w_sem.at[n])

    def wo_part(s, n):
        m = s * o_parts + n
        return wv.at[lax.div(m, per), pl.ds(pl.multiple_of(lax.rem(m, per) * o_rows, o_rows), o_rows)]

    def wo_copy(s, n):
        src = wo_ref.at[pl.ds(pl.multiple_of(s * o_rows, o_rows), o_rows), pl.ds(n * o_cols, o_cols)]
        return pltpu.make_async_copy(src, wo_part(s, n), wo_sem.at[s])

    def w_start(n):
        for t in range(3):
            w_copy(n, t).start()

    def arrived(ref, sem):
        pltpu.make_async_copy(ref, ref, sem).wait()

    n_dev = n_cx * n_cy
    barrier = pltpu.get_barrier_semaphore()

    def greet(k, _):
        other = lax.rem(i * n_cy + j + k, n_dev)
        pl.semaphore_signal(barrier, inc=1, device_id={"cx": lax.div(other, n_cy), "cy": lax.rem(other, n_cy)},
                            device_id_type=MESH)
        return 0

    lax.fori_loop(1, n_dev // 2, greet, 0)
    w_start(0)
    lax.fori_loop(n_dev // 2, n_dev, greet, 0)
    w_start(1)

    low = lax.broadcasted_iota(jnp.int32, (rows, 128), 1) < hd
    low_o = low[:rows // 2]
    q_rows = rows // 2

    def slot(n):
        return lax.rem(n, GROUPS) * group

    def keeps(n, kk):
        return both(step(n)[1] + kk == e, par == c)

    def qkv_send(n, kk, r=None):
        s, first = step(n)
        src, dst = stage.at[s, slot(n) + kk], buf.at[s, par, pair]
        if r is not None:
            src, dst = src.at[r], dst.at[r]
        return pltpu.make_async_remote_copy(src, dst, qs_sem.at[s], qr_sem.at[s],
                                            device_id=dev(first + kk, par), device_id_type=MESH)

    def send(n, r=None):
        for m in ORDER:
            qkv_send(n, lax.rem(xx + m, group), r).start()
        own = lax.rem(xx, group)
        s = lax.div(n, GROUPS)

        @pl.when(keeps(n, own))
        def _():
            if r is None:
                buf[s, par, pair] = stage[s, slot(n) + own]
            else:
                buf[s, par, pair, r] = stage[s, slot(n) + own, r]

        @pl.when(jnp.logical_not(keeps(n, own)))
        def _():
            qkv_send(n, own, r).start()

    def pack(n, r, q, k, v):
        s, at = lax.div(n, GROUPS), slot(n)
        for p in range(group // 2):
            sl = slice(128 * p, 128 * p + 128)
            top, bot, kk, vv = q[:q_rows, sl], q[q_rows:, sl], k[:, sl], v[:, sl]
            stage[s, at + 2 * p, r, 0:q_rows] = jnp.where(low_o, top, pltpu.roll(bot, hd, 1)).astype(BF16)
            stage[s, at + 2 * p + 1, r, 0:q_rows] = jnp.where(low_o, pltpu.roll(top, hd, 1), bot).astype(BF16)
            stage[s, at + 2 * p, r, q_rows:] = jnp.where(low, kk, pltpu.roll(vv, hd, 1)).astype(BF16)
            stage[s, at + 2 * p + 1, r, q_rows:] = jnp.where(low, pltpu.roll(kk, hd, 1), vv).astype(BF16)

    def project_half(n, r):
        x_half = xv[pl.ds(pl.multiple_of(r * rows, rows), rows)]
        pack(n, r, *(jnp.dot(x_half, wv[3 * n + t], preferred_element_type=F32) for t in range(3)))

    def project(n):
        arrived(wv.at[pl.ds(3 * n, 3)], w_sem.at[n])
        q, k, v = (jnp.dot(xv[...], wv[3 * n + t], preferred_element_type=F32) for t in range(3))
        for r in range(2):
            half_rows = slice(r * rows, (r + 1) * rows)
            pack(n, r, q[half_rows], k[half_rows], v[half_rows])
        send(n)

    x_in.wait()
    arrived(wv.at[pl.ds(0, 3)], w_sem.at[0])
    w_start(2)
    w_start(3)
    project_half(0, c)
    pl.semaphore_wait(barrier, n_dev - 1)
    x_swap = pltpu.make_async_remote_copy(xv.at[my_rows], xv.at[my_rows], xs_sem, xr_sem,
                                          device_id=dev(e, 1 - c), device_id_type=MESH)
    x_swap.start()
    send(0, c)
    for n in range(1, GROUPS):
        arrived(wv.at[pl.ds(3 * n, 3)], w_sem.at[n])
        for m in range(n + 3, min(steps, GROUPS + n + 3)):
            w_start(m)
        project_half(n, c)
        send(n, c)
    x_swap.wait()
    for n in range(GROUPS):
        project_half(n, 1 - c)
        send(n, 1 - c)

    local = both(lax.div(e, half) == c, par == c)

    def of(ref, count, less):
        def wait(sem):
            @pl.when(less)
            def _():
                arrived(ref.at[pl.ds(0, count - 1)], sem)

            @pl.when(jnp.logical_not(less))
            def _():
                arrived(ref, sem)
        return wait

    def fwd(s, core):
        part = buf.at[s, core, :, :, pl.ds(q_rows, rows)]
        return pltpu.make_async_remote_copy(part, part, fs_sem.at[s], fr_sem.at[s],
                                            device_id=dev(e, 1 - c), device_id_type=MESH)

    def forward(s):
        of(buf.at[s, c], half, local)(qr_sem.at[s])
        fwd(s, c).start()

    key_chips = half // KEY_PARTS

    def attend(s):
        qs = []
        for n in range(half):
            for r in range(2):
                qq = buf[s, c, n, r, 0:q_rows].astype(F32)
                qs.append(jnp.where(low_o, qq, 0.0).astype(BF16))
                qs.append(jnp.where(low_o, pltpu.roll(qq, hd, 1), 0.0).astype(BF16))
        q = jnp.concatenate(qs, axis=0)
        m = den = o = None
        for side in range(2):
            core = c if side == 0 else 1 - c
            if side == 1:
                fwd(s, 1 - c).wait_recv()
            for g in range(KEY_PARTS):
                kv = jnp.concatenate([buf[s, core, g * key_chips + n, r, q_rows:]
                                      for n in range(key_chips) for r in range(2)], axis=0)
                logits = lax.dot_general(q, kv, (((1,), (1,)), ((), ())), preferred_element_type=F32)
                top = jnp.max(logits, axis=1, keepdims=True)
                new = top if m is None else jnp.maximum(m, top)
                w = jnp.exp2((logits - new) * scale)
                part = jnp.sum(w, axis=1, keepdims=True)
                wkv = jnp.dot(w.astype(BF16), kv, preferred_element_type=F32)
                if m is None:
                    den, o = part, wkv
                else:
                    old = jnp.exp2((m - new) * scale)
                    den, o = den * old + part, o * old + wkv
                m = new
        o = o / den
        hr = rows // 2
        for u in range(chips):
            lo, hi = o[u * rows:u * rows + hr], o[u * rows + hr:(u + 1) * rows]
            ostage[s, u] = jnp.where(low_o, pltpu.roll(lo, hd, 1), hi).astype(BF16)

        cols = row_chips // 2
        for dy in list(range(1, n_cx)) + [0]:
            row = lax.rem(i + dy, n_cx)
            for m in range(2 * cols):
                col, core = m // 2, m % 2
                u = row * 2 * cols + m
                copy = pltpu.make_async_remote_copy(
                    ostage.at[s, u], obuf.at[s, e], os_sem.at[s], or_sem.at[s, lax.div(e, half)],
                    device_id={"cx": row, "cy": 4 * col + 2 * c + core}, device_id_type=MESH)
                if dy:
                    copy.start()
                    continue
                stays = both(both(col == lax.div(xx, 2), par == c), core == c)

                @pl.when(stays)
                def _():
                    obuf[s, e] = ostage[s, u]

                @pl.when(jnp.logical_not(stays))
                def _():
                    copy.start()

    def output(s, last=False):
        arrived(wv.at[pl.ds(s * (o_parts // per), o_parts // per)], wo_sem.at[s])
        for h in range(2):
            of(obuf.at[s, pl.ds(h * half, half)], half, both(par == c, lax.div(e, half) == h))(or_sem.at[s, h])
            tiles = []
            for p in range(half // 2):
                a, b = (obuf[s, h * half + 2 * p + q].astype(F32) for q in range(2))
                top = jnp.where(low_o, a, pltpu.roll(b, hd, 1))
                bot = jnp.where(low_o, pltpu.roll(a, hd, 1), b)
                tiles.append(jnp.concatenate([top, bot], axis=0).astype(BF16))
            o = jnp.concatenate(tiles, axis=1)
            depth = slice(h * half * hd, (h + 1) * half * hd)
            for n in range(o_parts):
                cols = slice(n * o_cols, (n + 1) * o_cols)
                total = acc[:, cols] + jnp.dot(o, wo_part(s, n)[depth], preferred_element_type=F32)
                if last and h:
                    y_ref[:, cols] = total.astype(BF16)
                else:
                    acc[:, cols] = total

    def project_loop(n, _):
        project(n)
        return 0

    lax.fori_loop(GROUPS, steps, project_loop, 0)
    for s in range(chunks):
        for n in range(o_parts):
            wo_copy(s, n).start()
    acc[...] = jnp.zeros_like(acc)

    def chunk_loop(s, _):
        forward(s)
        attend(s)
        return 0

    lax.fori_loop(0, chunks, chunk_loop, 0)
    for s in range(chunks - 1):
        output(s)
    output(chunks - 1, last=True)

    for s in range(chunks):
        of(stage.at[s], half, local)(qs_sem.at[s])
        fwd(s, c).wait_send()
        of(ostage.at[s], chips, par == c)(os_sem.at[s])


def solution(mesh):
    n_cx, n_cy = mesh.shape["cx"], mesh.shape["cy"]
    chips = n_cx * n_cy // 2

    def attend_local(x_blk, w_qkv, w_o):
        heads, hd, width = w_o.shape
        rows = x_blk.shape[1]
        chunks = heads // chips
        half = chips // 2
        group = half // GROUPS
        steps = chunks * GROUPS
        dma, vm = pltpu.SemaphoreType.DMA, pltpu.VMEM
        y = pl.pallas_call(
            functools.partial(kernel, (n_cx, n_cy, chips, chunks, heads, hd)),
            out_shape=pltpu.VMEM((rows, width), BF16),
            in_specs=[pl.BlockSpec(memory_space=pltpu.HBM)] * 3,
            out_specs=pl.BlockSpec(memory_space=pltpu.VMEM),
            scratch_shapes=[
                vm((2 * rows, width), BF16),
                vm((3 * steps, width, group * hd), BF16),
                vm((chunks, half, 2, 3 * rows // 2, 128), BF16),
                vm((chunks, 2, half, 2, 3 * rows // 2, 128), BF16),
                vm((chunks, chips, rows // 2, 128), BF16),
                vm((chunks, chips, rows // 2, 128), BF16),
                vm((rows, width), F32),
                dma, dma((steps,)), dma((chunks,)), dma, dma,
                dma((chunks,)), dma((chunks,)), dma((chunks,)), dma((chunks,)), dma((chunks,)), dma((chunks, 2)),
            ],
            compiler_params=pltpu.CompilerParams(
                collective_id=0, has_side_effects=True, vmem_limit_bytes=56 * 2 ** 20),
        )(x_blk[0], w_qkv, w_o.reshape(heads * hd, width))
        return y[None]

    return jax.shard_map(
        attend_local, mesh=mesh,
        in_specs=(P("dp", ("cx", "cy"), None), P(None, None), P(None, None, None)),
        out_specs=P("dp", ("cx", "cy"), None), check_vma=False)
```

```python
import functools

import jax
import jax.numpy as jnp
from jax import lax
from jax.experimental import pallas as pl
from jax.experimental.pallas import tpu as pltpu
from jax.sharding import PartitionSpec as P

MESH = pl.DeviceIdType.MESH
BF16, F32 = jnp.bfloat16, jnp.float32
LOG2E = 1.4426950408889634
GROUPS = 2
KEY_PARTS = 2
ORDER = (1, 3, 2)


def both(a, b):
    return jnp.logical_and(a, b)


def kernel(cfg, x_ref, w_ref, wo_ref, y_ref, xv, wv, stage, buf, ostage, obuf, acc,
           x_sem, w_sem, wo_sem, xs_sem, xr_sem, qs_sem, qr_sem, fs_sem, fr_sem, os_sem, or_sem):
    n_cx, n_cy, chips, chunks, heads, hd = cfg
    row_chips = n_cy // 2
    half = chips // 2
    rows, width = x_ref.shape
    span = half * hd
    scale = hd ** -0.5 * LOG2E
    group = half // GROUPS
    steps = chunks * GROUPS
    o_rows = chips * hd
    o_cols = group * hd
    o_parts = width // o_cols
    per = width // o_rows

    i = lax.axis_index("cx")
    j = lax.axis_index("cy")
    xx = lax.div(j, 2)
    c = lax.rem(j, 2)
    e = i * row_chips + xx
    par = lax.rem(e, 2)
    pair = lax.div(e, 2)

    def dev(chip, core):
        return {"cx": lax.div(chip, row_chips), "cy": lax.rem(chip, row_chips) * 2 + core}

    my_rows = pl.ds(pl.multiple_of(c * rows, rows), rows)
    x_in = pltpu.make_async_copy(x_ref, xv.at[my_rows], x_sem)
    x_in.start()

    def step(n):
        return lax.div(n, GROUPS), c * half + lax.rem(lax.rem(n, GROUPS) + i, GROUPS) * group

    def w_copy(n, t):
        s, first = step(n)
        col = pl.multiple_of((t * heads + s * chips + first) * hd, 128)
        return pltpu.make_async_copy(w_ref.at[:, pl.ds(col, group * hd)], wv.at[3 * n + t], w_sem.at[n])

    def wo_part(s, n):
        m = s * o_parts + n
        return wv.at[lax.div(m, per), pl.ds(pl.multiple_of(lax.rem(m, per) * o_rows, o_rows), o_rows)]

    def wo_copy(s, n):
        src = wo_ref.at[pl.ds(pl.multiple_of(s * o_rows, o_rows), o_rows), pl.ds(n * o_cols, o_cols)]
        return pltpu.make_async_copy(src, wo_part(s, n), wo_sem.at[s])

    def w_start(n):
        for t in range(3):
            w_copy(n, t).start()

    def arrived(ref, sem):
        pltpu.make_async_copy(ref, ref, sem).wait()

    n_dev = n_cx * n_cy
    barrier = pltpu.get_barrier_semaphore()

    def greet(k, _):
        other = lax.rem(i * n_cy + j + k, n_dev)
        pl.semaphore_signal(barrier, inc=1, device_id={"cx": lax.div(other, n_cy), "cy": lax.rem(other, n_cy)},
                            device_id_type=MESH)
        return 0

    lax.fori_loop(1, n_dev // 2, greet, 0)
    w_start(0)
    lax.fori_loop(n_dev // 2, n_dev, greet, 0)
    w_start(1)

    low = lax.broadcasted_iota(jnp.int32, (rows, 128), 1) < hd
    low_o = low[:rows // 2]
    q_rows = rows // 2

    def slot(n):
        return lax.rem(n, GROUPS) * group

    def keeps(n, kk):
        return both(step(n)[1] + kk == e, par == c)

    def qkv_send(n, kk, r=None):
        s, first = step(n)
        src, dst = stage.at[s, slot(n) + kk], buf.at[s, par, pair]
        if r is not None:
            src, dst = src.at[r], dst.at[r]
        return pltpu.make_async_remote_copy(src, dst, qs_sem.at[s], qr_sem.at[s],
                                            device_id={"cx": lax.div(first, row_chips), "cy": 2 * kk + par},
                                            device_id_type=MESH)

    def send(n, r=None):
        for m in ORDER:
            qkv_send(n, lax.rem(xx + m, group), r).start()
        own = lax.rem(xx, group)
        s = lax.div(n, GROUPS)

        @pl.when(keeps(n, own))
        def _():
            if r is None:
                buf[s, par, pair] = stage[s, slot(n) + own]
            else:
                buf[s, par, pair, r] = stage[s, slot(n) + own, r]

        @pl.when(jnp.logical_not(keeps(n, own)))
        def _():
            qkv_send(n, own, r).start()

    def pack(n, r, q, k, v):
        s, at = lax.div(n, GROUPS), slot(n)
        for p in range(group // 2):
            sl = slice(128 * p, 128 * p + 128)
            top, bot, kk, vv = q[:q_rows, sl], q[q_rows:, sl], k[:, sl], v[:, sl]
            stage[s, at + 2 * p, r, 0:q_rows] = jnp.where(low_o, top, pltpu.roll(bot, hd, 1)).astype(BF16)
            stage[s, at + 2 * p + 1, r, 0:q_rows] = jnp.where(low_o, pltpu.roll(top, hd, 1), bot).astype(BF16)
            stage[s, at + 2 * p, r, q_rows:] = jnp.where(low, kk, pltpu.roll(vv, hd, 1)).astype(BF16)
            stage[s, at + 2 * p + 1, r, q_rows:] = jnp.where(low, pltpu.roll(kk, hd, 1), vv).astype(BF16)

    def project_half(n, r):
        x_half = xv[pl.ds(pl.multiple_of(r * rows, rows), rows)]
        pack(n, r, *(jnp.dot(x_half, wv[3 * n + t], preferred_element_type=F32) for t in range(3)))

    def project(n):
        arrived(wv.at[pl.ds(3 * n, 3)], w_sem.at[n])
        q, k, v = (jnp.dot(xv[...], wv[3 * n + t], preferred_element_type=F32) for t in range(3))
        for r in range(2):
            half_rows = slice(r * rows, (r + 1) * rows)
            pack(n, r, q[half_rows], k[half_rows], v[half_rows])
        send(n)

    x_in.wait()
    arrived(wv.at[pl.ds(0, 3)], w_sem.at[0])
    w_start(2)
    w_start(3)
    project_half(0, c)
    pl.semaphore_wait(barrier, n_dev - 1)
    x_swap = pltpu.make_async_remote_copy(xv.at[my_rows], xv.at[my_rows], xs_sem, xr_sem,
                                          device_id=dev(e, 1 - c), device_id_type=MESH)
    x_swap.start()
    send(0, c)
    for n in range(1, GROUPS):
        arrived(wv.at[pl.ds(3 * n, 3)], w_sem.at[n])
        for m in range(n + 3, min(steps, GROUPS + n + 3)):
            w_start(m)
        project_half(n, c)
        send(n, c)
    x_swap.wait()
    for n in range(GROUPS):
        project_half(n, 1 - c)
        send(n, 1 - c)

    local = both(lax.div(e, half) == c, par == c)

    def of(ref, count, less):
        def wait(sem):
            @pl.when(less)
            def _():
                arrived(ref.at[pl.ds(0, count - 1)], sem)

            @pl.when(jnp.logical_not(less))
            def _():
                arrived(ref, sem)
        return wait

    def fwd(s, core):
        part = buf.at[s, core, :, :, pl.ds(q_rows, rows)]
        return pltpu.make_async_remote_copy(part, part, fs_sem.at[s], fr_sem.at[s],
                                            device_id=dev(e, 1 - c), device_id_type=MESH)

    def forward(s):
        of(buf.at[s, c], half, local)(qr_sem.at[s])
        fwd(s, c).start()

    key_chips = half // KEY_PARTS

    def attend(s):
        qs = []
        for n in range(half):
            for r in range(2):
                qq = buf[s, c, n, r, 0:q_rows].astype(F32)
                qs.append(jnp.where(low_o, qq, 0.0).astype(BF16))
                qs.append(jnp.where(low_o, pltpu.roll(qq, hd, 1), 0.0).astype(BF16))
        q = jnp.concatenate(qs, axis=0)
        m = den = o = None
        for side in range(2):
            core = c if side == 0 else 1 - c
            if side == 1:
                fwd(s, 1 - c).wait_recv()
            for g in range(KEY_PARTS):
                kv = jnp.concatenate([buf[s, core, g * key_chips + n, r, q_rows:]
                                      for n in range(key_chips) for r in range(2)], axis=0)
                logits = lax.dot_general(q, kv, (((1,), (1,)), ((), ())), preferred_element_type=F32)
                top = jnp.max(logits, axis=1, keepdims=True)
                new = top if m is None else jnp.maximum(m, top)
                w = jnp.exp2((logits - new) * scale)
                part = jnp.sum(w, axis=1, keepdims=True)
                wkv = jnp.dot(w.astype(BF16), kv, preferred_element_type=F32)
                if m is None:
                    den, o = part, wkv
                else:
                    old = jnp.exp2((m - new) * scale)
                    den, o = den * old + part, o * old + wkv
                m = new
        o = o / den
        hr = rows // 2
        for u in range(chips):
            lo, hi = o[u * rows:u * rows + hr], o[u * rows + hr:(u + 1) * rows]
            ostage[s, u] = jnp.where(low_o, pltpu.roll(lo, hd, 1), hi).astype(BF16)

        cols = row_chips // 2
        for dy in list(range(1, n_cx)) + [0]:
            row = lax.rem(i + dy, n_cx)
            for m in range(2 * cols):
                col, core = m // 2, m % 2
                u = row * 2 * cols + m
                copy = pltpu.make_async_remote_copy(
                    ostage.at[s, u], obuf.at[s, e], os_sem.at[s], or_sem.at[s, lax.div(e, half)],
                    device_id={"cx": row, "cy": 4 * col + 2 * c + core}, device_id_type=MESH)
                if dy:
                    copy.start()
                    continue
                stays = both(both(col == lax.div(xx, 2), par == c), core == c)

                @pl.when(stays)
                def _():
                    obuf[s, e] = ostage[s, u]

                @pl.when(jnp.logical_not(stays))
                def _():
                    copy.start()

    def output(s, last=False):
        arrived(wv.at[pl.ds(s * (o_parts // per), o_parts // per)], wo_sem.at[s])
        for h in range(2):
            of(obuf.at[s, pl.ds(h * half, half)], half, both(par == c, lax.div(e, half) == h))(or_sem.at[s, h])
            tiles = []
            for p in range(half // 2):
                a, b = (obuf[s, h * half + 2 * p + q].astype(F32) for q in range(2))
                top = jnp.where(low_o, a, pltpu.roll(b, hd, 1))
                bot = jnp.where(low_o, pltpu.roll(a, hd, 1), b)
                tiles.append(jnp.concatenate([top, bot], axis=0).astype(BF16))
            o = jnp.concatenate(tiles, axis=1)
            depth = slice(h * half * hd, (h + 1) * half * hd)
            for n in range(o_parts):
                cols = slice(n * o_cols, (n + 1) * o_cols)
                total = acc[:, cols] + jnp.dot(o, wo_part(s, n)[depth], preferred_element_type=F32)
                if last and h:
                    y_ref[:, cols] = total.astype(BF16)
                else:
                    acc[:, cols] = total

    def project_loop(n, _):
        project(n)
        return 0

    lax.fori_loop(GROUPS, steps, project_loop, 0)
    for s in range(chunks):
        for n in range(o_parts):
            wo_copy(s, n).start()
    acc[...] = jnp.zeros_like(acc)

    def chunk_loop(s, _):
        forward(s)
        attend(s)
        return 0

    lax.fori_loop(0, chunks, chunk_loop, 0)
    for s in range(chunks - 1):
        output(s)
    output(chunks - 1, last=True)

    for s in range(chunks):
        of(stage.at[s], half, local)(qs_sem.at[s])
        fwd(s, c).wait_send()
        of(ostage.at[s], chips, par == c)(os_sem.at[s])


def solution(mesh):
    n_cx, n_cy = mesh.shape["cx"], mesh.shape["cy"]
    chips = n_cx * n_cy // 2

    def attend_local(x_blk, w_qkv, w_o):
        heads, hd, width = w_o.shape
        rows = x_blk.shape[1]
        chunks = heads // chips
        half = chips // 2
        group = half // GROUPS
        assert group == n_cy // 2
        steps = chunks * GROUPS
        dma, vm = pltpu.SemaphoreType.DMA, pltpu.VMEM
        y = pl.pallas_call(
            functools.partial(kernel, (n_cx, n_cy, chips, chunks, heads, hd)),
            out_shape=pltpu.VMEM((rows, width), BF16),
            in_specs=[pl.BlockSpec(memory_space=pltpu.HBM)] * 3,
            out_specs=pl.BlockSpec(memory_space=pltpu.VMEM),
            scratch_shapes=[
                vm((2 * rows, width), BF16),
                vm((3 * steps, width, group * hd), BF16),
                vm((chunks, half, 2, 3 * rows // 2, 128), BF16),
                vm((chunks, 2, half, 2, 3 * rows // 2, 128), BF16),
                vm((chunks, chips, rows // 2, 128), BF16),
                vm((chunks, chips, rows // 2, 128), BF16),
                vm((rows, width), F32),
                dma, dma((steps,)), dma((chunks,)), dma, dma,
                dma((chunks,)), dma((chunks,)), dma((chunks,)), dma((chunks,)), dma((chunks,)), dma((chunks, 2)),
            ],
            compiler_params=pltpu.CompilerParams(
                collective_id=0, has_side_effects=True, vmem_limit_bytes=56 * 2 ** 20),
        )(x_blk[0], w_qkv, w_o.reshape(heads * hd, width))
        return y[None]

    return jax.shard_map(
        attend_local, mesh=mesh,
        in_specs=(P("dp", ("cx", "cy"), None), P(None, None), P(None, None, None)),
        out_specs=P("dp", ("cx", "cy"), None), check_vma=False)
```
